512 devices in a mesh: member: 2 (over y), lon: 128 (over z, x), lat: 2 (over core).
Axes of the slice: x: 4, y: 2, z: 32, core: 2. Of those that a mesh axis runs over, the one named last changes fastest.
The devices are a block of a 4x8x32 slice.
Arguments:
- state_tokens: bfloat16 [8, 24, 1536, 768], P('member', 'lat', 'lon'), parts along dimension 0, may hold values from -32 to 32
- land_mask: int32 [24, 1536], P('lat', 'lon'), may hold values 0 or 1
- pad_mask: int32 [24], replicated, may hold values from 0 to 1, as said below
- land_embed: float32 [2, 768], replicated, may hold values from -3 to 3
- w_qkv: bfloat16 [768, 1152], replicated, may hold values from -0.21875 to 0.21875
- w_proj: bfloat16 [384, 768], replicated, may hold values from -0.3125 to 0.3125
- proj_bias: float32 [768], replicated, may hold values from -4 to 4
- norm_gain: float32 [768], replicated, may hold values from 0.5 to 1.5
- norm_shift: float32 [768], replicated, may hold values from -1.5 to 1.5
- bias_table: bfloat16 [4, 2, 12, 3312], P('lat'), may hold values from -3.5 to 320
- index_table: int32 [144, 144], replicated, may hold values from 0 to 3311
Outputs:
- result: bfloat16 [8, 24, 1536, 768], P('member', 'lat', 'lon'), parts along dimension 0
The draws below stay inside these ranges and needn't reach their ends.
There are 2 independent parts, one for each index of `member`. The reference program is written for one: setup_inputs(seed, part) draws one part's arguments, and reference() takes and returns one part's arrays. A program takes and returns all parts, laid end to end along the dimension named above; an argument that names none is the same for every part. Nothing has to cross between parts.
Inputs may be any that keep to these rules, and one draw needn't show every extreme that they name: pad_mask is 1 on every row except at most the first 2 and the last 2 of the 24 rows, which are 0 where padded; one of the two ends has exactly 2 padding rows.
All inputs are finite; a program needn't handle non-finite values. No bound on the sum of `land_mask` on one device may be relied on, other than what follows from the above.
Results may differ from the reference program's by a relative error of at most 0.0085.
Values may be sent and summed in bfloat16 or wider, within the bound.
A program may use at most 64 MiB of HBM per device.

```python
import jax
import jax.numpy as jnp
from jax import lax

D = 768
HEADS = 12
HEAD_DIM = 32
WIN_Z = 2
WIN_LAT = 6
WIN_LON = 12
LEVELS = 4
WIN_TOK = 144
BIAS_POS = 3312
LAT = 24
LON = 1536
LAT_WIN = 4
Z_WIN = 2


def index_helper(key):
    return jax.random.randint(jax.random.fold_in(key, 11), (WIN_TOK, WIN_TOK), 0, BIAS_POS, dtype=jnp.int32)


def draw_index_table(key, part):
    return index_helper(key)


def draw_bias_table(key, part):
    inner_key = jax.random.fold_in(key, 23)
    full_shape = (LAT_WIN, Z_WIN, HEADS, BIAS_POS)
    entries = jnp.clip(jax.random.normal(inner_key, full_shape, jnp.float32), -3.5, 3.5)
    return entries.astype(jnp.bfloat16)


def draw_state_tokens(key, part):
    subkeys = jax.random.split(jax.random.fold_in(key, 5), 3)
    full_shape = (LEVELS, LAT, LON, D)
    normal_part = jnp.clip(jax.random.normal(subkeys[0], full_shape, jnp.float32), -3.5, 3.5)
    row_scale = jnp.exp(jax.random.uniform(subkeys[1], (LEVELS, LAT, LON, 1), jnp.float32, jnp.log(0.3), jnp.log(3.0)))
    column_scale = jnp.exp(jax.random.uniform(subkeys[2], (D,), jnp.float32, jnp.log(0.3), jnp.log(3.0)))
    drawn_values = normal_part * row_scale * column_scale
    return drawn_values.astype(jnp.bfloat16)


def draw_pad_mask(key, part):
    subkeys = jax.random.split(jax.random.fold_in(key, 31), 2)
    other_end = jax.random.randint(subkeys[0], (), 0, 3, dtype=jnp.int32)
    chosen = jax.random.randint(subkeys[1], (), 0, 2, dtype=jnp.int32)
    north_rows = jnp.where(chosen == 0, 2, other_end)
    south_rows = jnp.where(chosen == 0, other_end, 2)
    positions = jnp.arange(LAT, dtype=jnp.int32)
    row_mask = (positions >= north_rows) & (positions < LAT - south_rows)
    return row_mask.astype(jnp.int32)


def place_ends(result, rng, smallest, high):
    spot = [jax.random.randint(jax.random.fold_in(rng, axis), (), 0, length) for axis, length in enumerate(result.shape)]
    main_axis = result.shape.index(max(result.shape))
    neighbour = spot[:main_axis] + [(spot[main_axis] + 1) % result.shape[main_axis]] + spot[main_axis + 1:]
    return result.at[tuple(spot)].set(smallest).at[tuple(neighbour)].set(high)


def scatter_about(own_key, extent, width, bound, held_as=jnp.bfloat16):
    return jnp.clip(width * jax.random.normal(own_key, extent, jnp.float32), -bound, bound).astype(held_as)


def setup_inputs(seed: int = 0, part: int = 0) -> dict:
    seeds = jax.random.split(jax.random.key(seed), 12)
    part_splits = jax.random.split(jax.random.fold_in(seeds[11], part), 12)
    state_tokens = draw_state_tokens(jax.random.fold_in(jax.random.fold_in(seeds[11], part), 71), part)
    land_mask = place_ends((jax.random.randint(seeds[1], (LAT, LON), 0, 3) < 1).astype(jnp.int32), jax.random.fold_in(seeds[1], 1), 0, 1)
    pad_mask = draw_pad_mask(jax.random.fold_in(seeds[11], 71), part)
    land_embed = scatter_about(seeds[3], (2, D), 0.5, 3.0, jnp.float32)
    w_qkv = scatter_about(seeds[4], (D, 3 * HEADS * HEAD_DIM), D ** -0.5, 0.21875)
    w_proj = scatter_about(seeds[5], (HEADS * HEAD_DIM, D), (HEADS * HEAD_DIM) ** -0.5, 0.3125)
    proj_bias = scatter_about(seeds[6], (D,), 1.0, 4.0, jnp.float32)
    norm_gain = jnp.clip(1.0 + 0.1 * jax.random.normal(seeds[7], (D,), jnp.float32), 0.5, 1.5)
    norm_shift = scatter_about(seeds[8], (D,), 0.3, 1.5, jnp.float32)
    bias_table = draw_bias_table(jax.random.fold_in(seeds[11], 71), part)
    index_table = draw_index_table(jax.random.fold_in(seeds[11], 71), part)
    return dict(state_tokens=state_tokens, land_mask=land_mask, pad_mask=pad_mask, land_embed=land_embed, w_qkv=w_qkv, w_proj=w_proj, proj_bias=proj_bias, norm_gain=norm_gain, norm_shift=norm_shift, bias_table=bias_table, index_table=index_table)


norm_epsilon = 1e-05

def region_of(position, length, window):
    half_window = window // 2
    return jnp.where(position < length - window, 0, jnp.where(position < length - half_window, 1, 2)).astype(jnp.int32)

def window_rules(levels, lat_start, lat_rows, lat_total, pad_mask):
    tokens = jnp.arange(WIN_TOK, dtype=jnp.int32)
    level_offset = tokens // (WIN_LAT * WIN_LON)
    row_offset = tokens // WIN_LON % WIN_LAT
    level_index = jnp.arange(levels // WIN_Z, dtype=jnp.int32)[:, None] * WIN_Z + level_offset[None, :]
    row_index = lat_start + jnp.arange(lat_rows // WIN_LAT, dtype=jnp.int32)[:, None] * WIN_LAT + row_offset[None, :]
    region = region_of(level_index, levels, WIN_Z)[:, None, :] * 3 + region_of(row_index, lat_total, WIN_LAT)[None, :, :]
    source_row = (row_index + WIN_LAT // 2) % lat_total
    lookup = (source_row[:, :, None] == jnp.arange(lat_total, dtype=jnp.int32)[None, None, :]).astype(jnp.int32)
    usable = lax.optimization_barrier(jnp.sum(lookup * pad_mask[None, None, :], axis=-1)) == 1
    return (region[:, :, :, None] == region[:, :, None, :]) & usable[None, :, None, :]

def earth_bias(bias_table, index_table):
    gathered = jnp.take(bias_table, index_table, axis=3).astype(jnp.float32)
    return jnp.transpose(gathered, (1, 0, 2, 3, 4))

def to_windows(layout):
    levels, lat_rows, lon_columns, channels = layout.shape
    shaped = layout.reshape(levels // WIN_Z, WIN_Z, lat_rows // WIN_LAT, WIN_LAT, lon_columns // WIN_LON, WIN_LON, channels)
    shaped = shaped.transpose(0, 2, 4, 1, 3, 5, 6)
    return shaped.reshape(levels // WIN_Z, lat_rows // WIN_LAT, lon_columns // WIN_LON, WIN_TOK, channels)

def from_windows(window_tiles):
    z_windows, lat_windows, lon_windows, tokens, channels = window_tiles.shape
    shaped = window_tiles.reshape(z_windows, lat_windows, lon_windows, WIN_Z, WIN_LAT, WIN_LON, channels)
    shaped = shaped.transpose(0, 3, 1, 4, 2, 5, 6)
    return shaped.reshape(z_windows * WIN_Z, lat_windows * WIN_LAT, lon_windows * WIN_LON, channels)

def attend(projections, bias_full, allowed):
    pieces = projections.astype(jnp.float32).reshape(projections.shape[:-1] + (3, HEADS, HEAD_DIM))
    queries = pieces[..., 0, :, :]
    key_rows = pieces[..., 1, :, :]
    value_rows = pieces[..., 2, :, :]
    scores = jnp.einsum('abthd,abuhd->abhtu', queries, key_rows) / jnp.sqrt(jnp.float32(HEAD_DIM)) + bias_full
    scores = jnp.where(allowed[:, :, None], scores, -jnp.inf)
    largest = lax.optimization_barrier(jnp.max(scores, axis=-1, keepdims=True))
    powers = jnp.exp(scores - largest)
    weights = (powers / lax.optimization_barrier(jnp.sum(powers, axis=-1, keepdims=True))).astype(jnp.bfloat16)
    attended = jnp.einsum('abhtu,abuhd->abthd', weights.astype(jnp.float32), value_rows).astype(jnp.bfloat16)
    return attended.reshape(attended.shape[:3] + (HEADS * HEAD_DIM,))

def finish(attended, w_proj, proj_bias, norm_gain, norm_shift):
    projected = jnp.dot(attended, w_proj, preferred_element_type=jnp.float32) + proj_bias
    average = lax.optimization_barrier(jnp.mean(projected, axis=-1, keepdims=True))
    centered = projected - average
    spread = lax.optimization_barrier(jnp.mean(centered * centered, axis=-1, keepdims=True))
    return centered * lax.rsqrt(spread + norm_epsilon) * norm_gain + norm_shift

def reference(state_tokens, land_mask, pad_mask, land_embed, w_qkv, w_proj, proj_bias, norm_gain, norm_shift, bias_table, index_table):
    embedded = jnp.where(land_mask[:, :, None] == 1, land_embed[1], land_embed[0])
    hidden = (state_tokens.astype(jnp.float32) + embedded[None]).astype(jnp.bfloat16)
    shifted = jnp.roll(hidden, (-(WIN_Z // 2), -(WIN_LAT // 2), -(WIN_LON // 2)), axis=(0, 1, 2))
    windows = jnp.moveaxis(to_windows(shifted), 2, 0)
    bias_full = earth_bias(bias_table, index_table)
    allowed = window_rules(LEVELS, 0, LAT, LAT, pad_mask)

    def one_column(column_block):
        projections = jnp.dot(column_block, w_qkv, preferred_element_type=jnp.float32).astype(jnp.bfloat16)
        return finish(attend(projections, bias_full, allowed), w_proj, proj_bias, norm_gain, norm_shift)
    normed = lax.map(one_column, windows)
    layout = from_windows(jnp.moveaxis(normed, 0, 2))
    restored = jnp.roll(layout, (WIN_Z // 2, WIN_LAT // 2, WIN_LON // 2), axis=(0, 1, 2))
    return (hidden.astype(jnp.float32) + restored).astype(jnp.bfloat16)
```

```python
import functools

import jax
import jax.numpy as jnp
from jax import lax
from jax.experimental import pallas as pl
from jax.experimental.pallas import tpu as pltpu
from jax.sharding import PartitionSpec as P

HEADS = 12
HEAD_DIM = 32
WIDTH = HEADS * HEAD_DIM
WIN_Z = 2
WIN_LAT = 6
WIN_LON = 12
WIN_TOK = 144
HALF = 72
PIECE = 18
GROUP = 4
GROUPS = HEADS // GROUP
T_STEP = 16
SPAN = 256
NEG = -1e30

norm_epsilon = 1e-05

MESH = pl.DeviceIdType.MESH
F32 = jnp.float32
BF16 = jnp.bfloat16


def nt_dot(a, b):
    return lax.dot_general(a, b, (((1,), (1,)), ((), ())), preferred_element_type=F32)


def kernel(
    lat_total,
    blocks,
    state_ref,
    land_ref,
    embed_ref,
    index_ref,
    bias_table_ref,
    w_qkv_hbm,
    w_proj_hbm,
    proj_bias_ref,
    gain_ref,
    shift_ref,
    pad_ref,
    out_ref,
    tokens,
    m0_ref,
    m1_ref,
    ed_ref,
    table32,
    table_ref,
    ordered,
    idx_ref,
    w_qkv,
    w_proj,
    edge_in,
    halo0,
    halo1,
    haloe,
    q_buf,
    kv_buf,
    acc,
    bias,
    att0,
    att1,
    atte,
    atte_out,
    atte_in,
    w_sem,
    lat_send,
    lat_recv,
    lon_send,
    lon_recv,
):
    member = lax.axis_index("member")
    lon = lax.axis_index("lon")
    lat = lax.axis_index("lat")
    lon_size = lax.axis_size("lon")
    left = (member, lax.rem(lon + lon_size - 1, lon_size), lat)
    right = (member, lax.rem(lon + 1, lon_size), lat)
    partner = (member, lon, 1 - lat)

    wq_copy = pltpu.make_async_copy(w_qkv_hbm, w_qkv, w_sem.at[0])
    wq_copy.start()
    wp_copy = pltpu.make_async_copy(w_proj_hbm, w_proj, w_sem.at[1])
    wp_copy.start()

    barrier = pltpu.get_barrier_semaphore()
    for other in (left, right, partner):
        pl.semaphore_signal(barrier, inc=1, device_id=other, device_id_type=MESH)

    levels = state_ref.shape[0]
    eye = (
        lax.broadcasted_iota(jnp.int32, (WIN_LON, WIN_LON), 0)
        == lax.broadcasted_iota(jnp.int32, (WIN_LON, WIN_LON), 1)
    )
    land = nt_dot(jnp.where(eye, 1.0, 0.0).astype(BF16), land_ref[...].astype(F32).astype(BF16))

    def place_of(level, r):
        rolled = (level + levels - 1) % levels
        if r < 3:
            return 12 * PIECE + rolled * PIECE + r * 6
        if r < 9:
            return rolled * 2 * PIECE + (r - 3) * 6
        return 8 * PIECE + rolled * PIECE + (r - 9) * 6

    def prepare(row_range):
        for r in row_range:
            embedded = jnp.where(land[:, r : r + 1] == 1.0, embed_ref[1:2, :], embed_ref[0:1, :])
            for level in range(levels):
                full = state_ref[level, r].astype(F32) + embedded
                place = place_of(level, r)
                for half in range(2):
                    tokens[half, place : place + 6, :] = full[half * 6 : half * 6 + 6]

    prepare(range(3))
    ed_ref[...] = tokens[:, 12 * PIECE :, :].astype(BF16)
    prepare(range(9, 12))
    m1_ref[...] = tokens[:, 8 * PIECE : 12 * PIECE, :].astype(BF16)
    pl.semaphore_wait(barrier, 3)

    def remote(src, dst, send, recv, to):
        return pltpu.make_async_remote_copy(
            src_ref=src, dst_ref=dst, send_sem=send, recv_sem=recv, device_id=to, device_id_type=MESH
        )

    edge_copy = remote(ed_ref, edge_in, lat_send.at[0], lat_recv.at[0], partner)
    edge_copy.start()

    def lon_copies(own, halo, k):
        return [
            remote(own.at[0], halo.at[1], lon_send.at[2 * k], lon_recv.at[2 * k], left),
            remote(own.at[1], halo.at[0], lon_send.at[2 * k + 1], lon_recv.at[2 * k + 1], right),
        ]

    copies1 = lon_copies(m1_ref, halo1, 0)
    copiese = lon_copies(edge_in, haloe, 1)
    copies0 = lon_copies(m0_ref, halo0, 2)
    for c in copies1:
        c.start()

    prepare(range(3, 9))
    m0_ref[...] = tokens[:, : 8 * PIECE, :].astype(BF16)

    rows = 2 * 2 * HEADS
    positions = bias_table_ref.shape[3]
    for z in range(2):
        for b in range(2):
            for k in range(blocks):
                place = k * rows + (z * 2 + b) * HEADS
                stop = min(positions, (k + 1) * SPAN)
                part = bias_table_ref[b, z, :, k * SPAN : stop].astype(F32)
                if stop < (k + 1) * SPAN:
                    part = jnp.concatenate([part, jnp.zeros((HEADS, (k + 1) * SPAN - stop), F32)], axis=1)
                table32[place : place + HEADS, :] = part
    table_ref[...] = table32[...].astype(BF16)

    new = lax.broadcasted_iota(jnp.int32, (WIN_TOK, WIN_TOK), 0)
    old = lax.broadcasted_iota(jnp.int32, (WIN_TOK, WIN_TOK), 1)
    inside = new % HALF
    order = jnp.where(old == inside // 6 * WIN_LON + new // HALF * 6 + inside % 6, 1.0, 0.0).astype(BF16)

    def reorder(x):
        x = jnp.dot(order, x.astype(F32).astype(BF16), preferred_element_type=F32)
        return nt_dot(x.astype(BF16), order)

    index = index_ref[...]
    ordered[...] = (reorder(index >> 8) * SPAN + reorder(index & (SPAN - 1))).astype(jnp.int32)
    steps = WIN_TOK // T_STEP
    for i in range(T_STEP):
        idx_ref[:, i * WIN_TOK : (i + 1) * WIN_TOK] = ordered[i * steps : (i + 1) * steps, :]

    def bias_step(step, carry):
        for j in range(T_STEP * WIN_TOK // 256):
            lanes = slice(j * 256, (j + 1) * 256)
            picked = idx_ref[pl.ds(step, 1), lanes]
            low = jnp.broadcast_to(picked & (SPAN - 1), (SPAN, 256))
            hot = jnp.where(lax.broadcasted_iota(jnp.int32, (SPAN, 256), 0) == low, 1.0, 0.0).astype(BF16)
            high = jnp.broadcast_to(picked >> 8, (rows, 256))
            found = jnp.dot(table_ref[...], hot, preferred_element_type=F32)
            total = found[:rows]
            for k in range(1, blocks):
                total = jnp.where(high == k, found[k * rows : (k + 1) * rows], total)
            acc[:, lanes] = total
        for i in range(T_STEP):
            for c in range(2):
                offset = i * WIN_TOK + c * HALF
                base = offset // 128 * 128
                shift = offset - base
                if shift + HALF <= 128:
                    piece = acc[:, base : base + 128]
                    if shift:
                        piece = pltpu.roll(piece, 128 - shift, 1)
                else:
                    piece = pltpu.roll(acc[:, base : base + 256], 256 - shift, 1)[:, :128]
                bias[c, pl.ds(i * steps + step, rows, stride=WIN_TOK), :] = piece
        return carry

    edge_copy.wait_recv()
    for c in copiese:
        c.start()
    for c in copies0:
        c.start()

    lax.fori_loop(0, steps, bias_step, 0)

    wq_copy.wait()

    def rounded(x):
        return x.astype(BF16).astype(F32)

    def put_main(slot, both):
        for a in range(2):
            kv_buf[slot, a, 0] = both[a * HALF : (a + 1) * HALF]

    def put_piece(slot, both, rh):
        for level in range(4):
            start = (level % 2) * 2 * PIECE + rh * PIECE
            kv_buf[slot, level // 2, 1, start : start + PIECE, :] = both[level * PIECE : (level + 1) * PIECE]

    def put_query(half, both, rh):
        for level in range(4):
            start = (level % 2) * 2 * PIECE + rh * PIECE
            q_buf[half, level // 2, 1, start : start + PIECE, :] = both[level * PIECE : (level + 1) * PIECE]

    features = w_qkv.shape[0]
    own = jnp.concatenate(
        [ref[...].reshape(-1, features) for ref in (m0_ref, m1_ref, edge_in)], axis=0
    )
    full = rounded(jnp.dot(own, w_qkv[...], preferred_element_type=F32))
    for half in range(2):
        main = full[half * 2 * HALF : (half + 1) * 2 * HALF]
        for a in range(2):
            q_buf[half, a, 0] = main[a * HALF : (a + 1) * HALF, :WIDTH]
        put_main(half + 1, main[:, WIDTH:])
        for rh in range(2):
            part = full[(4 + 2 * rh + half) * HALF : (5 + 2 * rh + half) * HALF]
            put_query(half, part[:, :WIDTH], rh)
            put_piece(half + 1, part[:, WIDTH:], rh)

    lane = lax.broadcasted_iota(jnp.int32, (HALF, 128), 1)
    row = lax.broadcasted_iota(jnp.int32, (HALF, 128), 0)
    lane_head = lane // HEAD_DIM
    lat_start = lat * 2 * WIN_LAT

    def attend(a, b, half):
        valid = lane < HALF
        same_z = jnp.logical_or(a == 0, (lane // 36) == (row // 36))
        wraps = lat_start + b * WIN_LAT >= lat_total - WIN_LAT
        same_r = jnp.logical_or(jnp.logical_not(wraps), (lane // PIECE) % 2 == (row // PIECE) % 2)
        lane_row = lane % 36 // WIN_LAT
        usable = jnp.zeros((HALF, 128), jnp.int32)
        for r in range(WIN_LAT):
            value = pad_ref[lax.rem(lat_start + b * WIN_LAT + r + WIN_LAT // 2, lat_total)]
            usable = jnp.where(lane_row == r, value, usable)
        allowed = valid & same_z & same_r & (usable == 1)
        slot0 = 2 * half
        out = []
        zeros = jnp.zeros((128 - HALF, 128), F32)
        ones = jnp.ones((256, 128), BF16)
        query_half = 1 - half
        for g in range(GROUPS):
            cols = slice(g * 128, (g + 1) * 128)
            vcols = slice(WIDTH + g * 128, WIDTH + (g + 1) * 128)
            q = q_buf[half, a, b, :, cols]
            stacked = jnp.concatenate([jnp.where(lane_head == h, q, 0.0) for h in range(GROUP)], axis=0).astype(BF16)
            keys = jnp.concatenate(
                [kv_buf[slot0, a, b, :, cols], zeros, kv_buf[slot0 + 1, a, b, :, cols], zeros], axis=0
            ).astype(BF16)
            values = jnp.concatenate(
                [kv_buf[slot0, a, b, :, vcols], zeros, kv_buf[slot0 + 1, a, b, :, vcols], zeros], axis=0
            ).astype(BF16)
            values = jnp.concatenate([values, ones], axis=1)
            scores = nt_dot(stacked, keys)
            powers = []
            for h in range(GROUP):
                first = ((a * 2 + b) * HEADS + g * GROUP + h) * WIN_TOK + query_half * HALF
                parts = []
                for c in range(2):
                    s = scores[h * HALF : (h + 1) * HALF, c * 128 : (c + 1) * 128] * (HEAD_DIM**-0.5)
                    s = s + bias[c, pl.ds(pl.multiple_of(first, 8), HALF), :]
                    parts.append(jnp.where(allowed, s, NEG))
                largest = jnp.max(jnp.maximum(parts[0], parts[1]), axis=1, keepdims=True)
                powers.append(jnp.concatenate([jnp.exp(p - largest) for p in parts], axis=1))
            weights = jnp.concatenate(powers, axis=0).astype(BF16)
            product = jnp.dot(weights, values, preferred_element_type=F32)
            top = jnp.zeros((HALF, 128), F32)
            bottom = jnp.zeros((HALF, 128), F32)
            for h in range(GROUP):
                part = product[h * HALF : (h + 1) * HALF]
                top = jnp.where(lane_head == h, part[:, :128], top)
                bottom = jnp.where(lane_head == h, part[:, 128:], bottom)
            out.append(top / bottom)
        return jnp.concatenate(out, axis=1)

    for c in copies1 + copiese:
        c.wait_recv()
    other = jnp.concatenate([ref[...].reshape(-1, features) for ref in (halo1, haloe)], axis=0)
    full = rounded(jnp.dot(other, w_qkv[:, WIDTH:], preferred_element_type=F32))
    for c in range(2):
        for rh in range(2):
            put_piece(3 * c, full[(2 * rh + c) * HALF : (2 * rh + c + 1) * HALF], rh)

    def edge_unit(half, carry):
        for a in range(2):
            result = attend(a, 1, half)
            for k in range(2):
                att1[half, (2 * a + k) * PIECE : (2 * a + k + 1) * PIECE, :] = result[2 * k * PIECE : (2 * k + 1) * PIECE]
                atte[half, (2 * a + k) * PIECE : (2 * a + k + 1) * PIECE, :] = result[
                    (2 * k + 1) * PIECE : (2 * k + 2) * PIECE
                ]
        return carry

    lax.fori_loop(0, 2, edge_unit, 0)
    atte_out[...] = atte[...].astype(BF16)
    return_copy = remote(atte_out, atte_in, lat_send.at[1], lat_recv.at[1], partner)
    return_copy.start()

    for c in copies0:
        c.wait_recv()
    full = rounded(jnp.dot(halo0[...].reshape(-1, features), w_qkv[:, WIDTH:], preferred_element_type=F32))
    for c in range(2):
        put_main(3 * c, full[c * 2 * HALF : (c + 1) * 2 * HALF])

    def main_unit(unit, carry):
        half = unit % 2
        a = unit // 2
        att0[half, pl.ds(pl.multiple_of(a * HALF, 8), HALF), :] = attend(a, 0, half)
        return carry

    lax.fori_loop(0, 4, main_unit, 0)
    wp_copy.wait()

    def finish(attended, hidden):
        projected = jnp.dot(attended.astype(BF16), w_proj[...], preferred_element_type=F32) + proj_bias_ref[...][None]
        average = jnp.mean(projected, axis=-1, keepdims=True)
        centered = projected - average
        spread = jnp.mean(centered * centered, axis=-1, keepdims=True)
        normed = centered * lax.rsqrt(spread + norm_epsilon) * gain_ref[...][None] + shift_ref[...][None]
        return hidden.astype(F32) + normed

    def emit(row_range):
        for level in range(levels):
            for r in row_range:
                place = place_of(level, r)
                pair = [tokens[half, place : place + 6, :] for half in range(2)]
                out_ref[level, r] = jnp.concatenate(pair, axis=0).astype(BF16)

    for half in range(2):
        tokens[half, : 8 * PIECE] = finish(att0[half], m0_ref[half])
        tokens[half, 8 * PIECE : 12 * PIECE] = finish(att1[half], m1_ref[half])
    emit(range(3, 12))
    return_copy.wait_recv()
    for half in range(2):
        tokens[half, 12 * PIECE :] = finish(atte_in[half], ed_ref[half])
    emit(range(3))
    edge_copy.wait_send()
    return_copy.wait_send()
    for c in copies1 + copiese + copies0:
        c.wait_send()


def on_device(
    state_tokens,
    land_mask,
    pad_mask,
    land_embed,
    w_qkv,
    w_proj,
    proj_bias,
    norm_gain,
    norm_shift,
    bias_table,
    index_table,
):
    levels, lat_rows, lon_columns, features = state_tokens.shape
    lat_windows, z_windows, heads, positions = bias_table.shape
    lat_total = lat_rows * lax.axis_size("lat")
    half_columns = WIN_LON // 2
    blocks = -(-positions // SPAN)

    side = (2, levels * PIECE, features)
    main = (2, levels * 2 * PIECE, features)
    rows = z_windows * lat_windows * heads

    vmem = pl.BlockSpec(memory_space=pltpu.VMEM)
    anywhere = pl.BlockSpec(memory_space=pl.ANY)
    return pl.pallas_call(
        functools.partial(kernel, lat_total, blocks),
        out_shape=jax.ShapeDtypeStruct(state_tokens.shape, BF16),
        in_specs=[vmem] * 5 + [anywhere] * 2 + [vmem] * 3 + [pl.BlockSpec(memory_space=pltpu.SMEM)],
        out_specs=vmem,
        scratch_shapes=[
            pltpu.VMEM((2, 16 * PIECE, features), F32),
            pltpu.VMEM(main, BF16),
            pltpu.VMEM(side, BF16),
            pltpu.VMEM(side, BF16),
            pltpu.VMEM((blocks * rows, SPAN), F32),
            pltpu.VMEM((blocks * rows, SPAN), BF16),
            pltpu.VMEM((WIN_TOK, WIN_TOK), jnp.int32),
            pltpu.VMEM((WIN_TOK // T_STEP, T_STEP * WIN_TOK), jnp.int32),
            pltpu.VMEM(w_qkv.shape, BF16),
            pltpu.VMEM(w_proj.shape, BF16),
            pltpu.VMEM(side, BF16),
            pltpu.VMEM(main, BF16),
            pltpu.VMEM(side, BF16),
            pltpu.VMEM(side, BF16),
            pltpu.VMEM((2, 2, 2, HALF, WIDTH), F32),
            pltpu.VMEM((4, 2, 2, HALF, 2 * WIDTH), F32),
            pltpu.VMEM((rows, T_STEP * WIN_TOK + 128), F32),
            pltpu.VMEM((2, rows * WIN_TOK, 128), F32),
            pltpu.VMEM((2, 2 * HALF, WIDTH), F32),
            pltpu.VMEM((2, HALF, WIDTH), F32),
            pltpu.VMEM((2, HALF, WIDTH), F32),
            pltpu.VMEM((2, HALF, WIDTH), BF16),
            pltpu.VMEM((2, HALF, WIDTH), BF16),
            pltpu.SemaphoreType.DMA((2,)),
            pltpu.SemaphoreType.DMA((2,)),
            pltpu.SemaphoreType.DMA((2,)),
            pltpu.SemaphoreType.DMA((6,)),
            pltpu.SemaphoreType.DMA((6,)),
        ],
        compiler_params=pltpu.CompilerParams(
            collective_id=0, has_side_effects=True, vmem_limit_bytes=56 * 1024 * 1024
        ),
        name="window_layer",
    )(
        state_tokens,
        land_mask,
        land_embed,
        index_table,
        bias_table,
        w_qkv,
        w_proj,
        proj_bias,
        norm_gain,
        norm_shift,
        pad_mask,
    )


def solution(mesh):
    in_specs = (
        P("member", "lat", "lon", None),
        P("lat", "lon"),
        P(),
        P(),
        P(),
        P(),
        P(),
        P(),
        P(),
        P("lat", None, None, None),
        P(),
    )
    out_specs = P("member", "lat", "lon", None)
    return jax.shard_map(
        on_device, mesh=mesh, in_specs=in_specs, out_specs=out_specs, check_vma=False
    )
```

```python
import functools

import jax
import jax.numpy as jnp
from jax import lax
from jax.experimental import pallas as pl
from jax.experimental.pallas import tpu as pltpu
from jax.sharding import PartitionSpec as P

HEADS = 12
HEAD_DIM = 32
WIDTH = HEADS * HEAD_DIM
WIN_Z = 2
WIN_LAT = 6
WIN_LON = 12
WIN_TOK = 144
HALF = 72
PIECE = 18
GROUP = 4
GROUPS = HEADS // GROUP
T_STEP = 16
SPAN = 256
NEG = -1e30

norm_epsilon = 1e-05

MESH = pl.DeviceIdType.MESH
F32 = jnp.float32
BF16 = jnp.bfloat16


def nt_dot(a, b):
    return lax.dot_general(a, b, (((1,), (1,)), ((), ())), preferred_element_type=F32)


def kernel(
    lat_total,
    blocks,
    state_hbm,
    embed_hbm,
    index_hbm,
    bias_table_hbm,
    w_qkv_hbm,
    w_proj_hbm,
    proj_bias_hbm,
    gain_hbm,
    shift_hbm,
    land_ref,
    pad_ref,
    out_hbm,
    state_ref,
    embed_ref,
    index_ref,
    bias_table_ref,
    proj_bias_ref,
    gain_ref,
    shift_ref,
    out_ref,
    tokens,
    m0_ref,
    m1_ref,
    ed_ref,
    table32,
    table_ref,
    ordered,
    idx_ref,
    w_qkv,
    w_proj,
    edge_in,
    halo0,
    halo1,
    haloe,
    q_buf,
    kv_buf,
    acc,
    bias,
    att0,
    att1,
    atte,
    atte_out,
    atte_in,
    w_sem,
    out_sem,
    lat_send,
    lat_recv,
    lon_send,
    lon_recv,
):
    member = lax.axis_index("member")
    lon = lax.axis_index("lon")
    lat = lax.axis_index("lat")
    lon_size = lax.axis_size("lon")
    left = (member, lax.rem(lon + lon_size - 1, lon_size), lat)
    right = (member, lax.rem(lon + 1, lon_size), lat)
    partner = (member, lon, 1 - lat)

    barrier = pltpu.get_barrier_semaphore()
    for other in (left, right, partner):
        pl.semaphore_signal(barrier, inc=1, device_id=other, device_id_type=MESH)

    loads = [
        pltpu.make_async_copy(src, dst, w_sem.at[k])
        for k, (src, dst) in enumerate(
            [
                (embed_hbm, embed_ref),
                (state_hbm, state_ref),
                (index_hbm, index_ref),
                (bias_table_hbm, bias_table_ref),
                (w_qkv_hbm, w_qkv),
                (w_proj_hbm, w_proj),
                (proj_bias_hbm, proj_bias_ref),
                (gain_hbm, gain_ref),
                (shift_hbm, shift_ref),
            ]
        )
    ]
    for load in loads:
        load.start()

    levels = state_ref.shape[2]

    def place_of(r, half, c):
        if r < 3:
            return 12 * PIECE + r * 6 + c, PIECE
        if r < 9:
            return (r - 3) * 6 + c, 2 * PIECE
        return 8 * PIECE + (r - 9) * 6 + c, PIECE

    loads[0].wait()
    loads[1].wait()
    sea = jnp.broadcast_to(embed_ref[0:1, :], (levels, embed_ref.shape[1]))
    ground = jnp.broadcast_to(embed_ref[1:2, :], (levels, embed_ref.shape[1]))

    def prepare(row_range):
        for r in row_range:
            for half in range(2):
                for c in range(6):
                    column = half * 6 + c
                    embedded = jnp.where(land_ref[r, column] == 1, ground, sea)
                    full = state_ref[r, column].astype(F32) + embedded
                    place, step = place_of(r, half, c)
                    for k in range(0, full.shape[1], 128):
                        tokens[half, k // 128, pl.ds(place, levels, stride=step), :] = full[:, k : k + 128]

    def joined(half, start, stop):
        return jnp.concatenate([tokens[half, k, start:stop, :] for k in range(tokens.shape[1])], axis=1)

    def gathered(ref, start, stop):
        for half in range(2):
            ref[half] = joined(half, start, stop).astype(BF16)

    prepare(range(3))
    gathered(ed_ref, 12 * PIECE, 16 * PIECE)
    prepare(range(9, 12))
    gathered(m1_ref, 8 * PIECE, 12 * PIECE)
    pl.semaphore_wait(barrier, 3)

    def remote(src, dst, send, recv, to):
        return pltpu.make_async_remote_copy(
            src_ref=src, dst_ref=dst, send_sem=send, recv_sem=recv, device_id=to, device_id_type=MESH
        )

    edge_copy = remote(ed_ref, edge_in, lat_send.at[0], lat_recv.at[0], partner)
    edge_copy.start()

    def lon_copies(own, halo, k):
        return [
            remote(own.at[0], halo.at[1], lon_send.at[2 * k], lon_recv.at[2 * k], left),
            remote(own.at[1], halo.at[0], lon_send.at[2 * k + 1], lon_recv.at[2 * k + 1], right),
        ]

    copies1 = lon_copies(m1_ref, halo1, 0)
    copiese = lon_copies(edge_in, haloe, 1)
    copies0 = lon_copies(m0_ref, halo0, 2)
    for c in copies1:
        c.start()

    prepare(range(3, 9))
    gathered(m0_ref, 0, 8 * PIECE)

    rows = 2 * 2 * HEADS
    positions = bias_table_ref.shape[3]
    loads[3].wait()
    for b in range(2):
        for h in range(HEADS):
            both = bias_table_ref[b, h].astype(F32)
            for k in range(blocks * SPAN // 128):
                place = k // 2 * rows + b * HEADS + h
                stop = min(positions, (k + 1) * 128)
                part = both[:, k * 128 : stop]
                if stop < (k + 1) * 128:
                    part = jnp.concatenate([part, jnp.zeros((2, (k + 1) * 128 - stop), F32)], axis=1)
                table32[k % 2, pl.ds(place, 2, stride=2 * HEADS), :] = part
    table_ref[...] = jnp.concatenate([table32[0], table32[1]], axis=1).astype(BF16)

    new = lax.broadcasted_iota(jnp.int32, (WIN_TOK, WIN_TOK), 0)
    old = lax.broadcasted_iota(jnp.int32, (WIN_TOK, WIN_TOK), 1)
    inside = new % HALF
    order = jnp.where(old == inside // 6 * WIN_LON + new // HALF * 6 + inside % 6, 1.0, 0.0).astype(BF16)

    def reorder(x):
        x = jnp.dot(order, x.astype(F32).astype(BF16), preferred_element_type=F32)
        return nt_dot(x.astype(BF16), order)

    loads[2].wait()
    index = index_ref[...]
    ordered[...] = (reorder(index >> 8) * SPAN + reorder(index & (SPAN - 1))).astype(jnp.int32)
    steps = WIN_TOK // T_STEP
    for i in range(T_STEP):
        idx_ref[:, i * WIN_TOK : (i + 1) * WIN_TOK] = ordered[i * steps : (i + 1) * steps, :]

    def bias_step(step, carry):
        for j in range(T_STEP * WIN_TOK // 256):
            lanes = slice(j * 256, (j + 1) * 256)
            picked = idx_ref[pl.ds(step, 1), lanes]
            low = jnp.broadcast_to(picked & (SPAN - 1), (SPAN, 256))
            hot = jnp.where(lax.broadcasted_iota(jnp.int32, (SPAN, 256), 0) == low, 1.0, 0.0).astype(BF16)
            high = jnp.broadcast_to(picked >> 8, (rows, 256))
            found = jnp.dot(table_ref[...], hot, preferred_element_type=F32)
            total = found[:rows]
            for k in range(1, blocks):
                total = jnp.where(high == k, found[k * rows : (k + 1) * rows], total)
            acc[:, lanes] = total
        for i in range(T_STEP):
            for c in range(2):
                offset = i * WIN_TOK + c * HALF
                base = offset // 128 * 128
                shift = offset - base
                if shift + HALF <= 128:
                    piece = acc[:, base : base + 128]
                    if shift:
                        piece = pltpu.roll(piece, 128 - shift, 1)
                else:
                    piece = pltpu.roll(acc[:, base : base + 256], 256 - shift, 1)[:, :128]
                bias[c, pl.ds(i * steps + step, rows, stride=WIN_TOK), :] = piece
        return carry

    edge_copy.wait_recv()
    for c in copiese:
        c.start()
    for c in copies0:
        c.start()

    lax.fori_loop(0, steps, bias_step, 0)

    loads[4].wait()

    def rounded(x):
        return x.astype(BF16).astype(F32)

    def put_main(slot, both):
        for level in range(4):
            rolled = (level + 3) % 4
            start = (rolled % 2) * 2 * PIECE
            kv_buf[slot, rolled // 2, 0, start : start + 2 * PIECE, :] = both[
                level * 2 * PIECE : (level + 1) * 2 * PIECE
            ]

    def put_piece(slot, both, rh):
        for level in range(4):
            rolled = (level + 3) % 4
            start = (rolled % 2) * 2 * PIECE + rh * PIECE
            kv_buf[slot, rolled // 2, 1, start : start + PIECE, :] = both[level * PIECE : (level + 1) * PIECE]

    def put_query_main(half, both):
        for level in range(4):
            rolled = (level + 3) % 4
            start = (rolled % 2) * 2 * PIECE
            q_buf[half, rolled // 2, 0, start : start + 2 * PIECE, :] = both[
                level * 2 * PIECE : (level + 1) * 2 * PIECE
            ]

    def put_query(half, both, rh):
        for level in range(4):
            rolled = (level + 3) % 4
            start = (rolled % 2) * 2 * PIECE + rh * PIECE
            q_buf[half, rolled // 2, 1, start : start + PIECE, :] = both[level * PIECE : (level + 1) * PIECE]

    features = w_qkv.shape[0]
    own = jnp.concatenate(
        [ref[...].reshape(-1, features) for ref in (m0_ref, m1_ref, edge_in)], axis=0
    )
    full = rounded(jnp.dot(own, w_qkv[...], preferred_element_type=F32))
    for half in range(2):
        main = full[half * 2 * HALF : (half + 1) * 2 * HALF]
        put_query_main(half, main[:, :WIDTH])
        put_main(half + 1, main[:, WIDTH:])
        for rh in range(2):
            part = full[(4 + 2 * rh + half) * HALF : (5 + 2 * rh + half) * HALF]
            put_query(half, part[:, :WIDTH], rh)
            put_piece(half + 1, part[:, WIDTH:], rh)

    lane = lax.broadcasted_iota(jnp.int32, (HALF, 128), 1)
    row = lax.broadcasted_iota(jnp.int32, (HALF, 128), 0)
    lane_head = lane // HEAD_DIM
    lat_start = lat * 2 * WIN_LAT

    def attend(a, b, half):
        valid = lane < HALF
        same_z = jnp.logical_or(a == 0, (lane // 36) == (row // 36))
        wraps = lat_start + b * WIN_LAT >= lat_total - WIN_LAT
        same_r = jnp.logical_or(jnp.logical_not(wraps), (lane // PIECE) % 2 == (row // PIECE) % 2)
        lane_row = lane % 36 // WIN_LAT
        usable = jnp.zeros((HALF, 128), jnp.int32)
        for r in range(WIN_LAT):
            value = pad_ref[lax.rem(lat_start + b * WIN_LAT + r + WIN_LAT // 2, lat_total)]
            usable = jnp.where(lane_row == r, value, usable)
        allowed = valid & same_z & same_r & (usable == 1)
        slot0 = 2 * half
        out = []
        zeros = jnp.zeros((128 - HALF, 128), F32)
        ones = jnp.ones((256, 128), BF16)
        query_half = 1 - half
        for g in range(GROUPS):
            cols = slice(g * 128, (g + 1) * 128)
            vcols = slice(WIDTH + g * 128, WIDTH + (g + 1) * 128)
            q = q_buf[half, a, b, :, cols]
            stacked = jnp.concatenate([jnp.where(lane_head == h, q, 0.0) for h in range(GROUP)], axis=0).astype(BF16)
            keys = jnp.concatenate(
                [kv_buf[slot0, a, b, :, cols], zeros, kv_buf[slot0 + 1, a, b, :, cols], zeros], axis=0
            ).astype(BF16)
            values = jnp.concatenate(
                [kv_buf[slot0, a, b, :, vcols], zeros, kv_buf[slot0 + 1, a, b, :, vcols], zeros], axis=0
            ).astype(BF16)
            values = jnp.concatenate([values, ones], axis=1)
            scores = nt_dot(stacked, keys)
            powers = []
            for h in range(GROUP):
                first = ((a * 2 + b) * HEADS + g * GROUP + h) * WIN_TOK + query_half * HALF
                parts = []
                for c in range(2):
                    s = scores[h * HALF : (h + 1) * HALF, c * 128 : (c + 1) * 128] * (HEAD_DIM**-0.5)
                    s = s + bias[c, pl.ds(pl.multiple_of(first, 8), HALF), :]
                    parts.append(jnp.where(allowed, s, NEG))
                largest = jnp.max(jnp.maximum(parts[0], parts[1]), axis=1, keepdims=True)
                powers.append(jnp.concatenate([jnp.exp(p - largest) for p in parts], axis=1))
            weights = jnp.concatenate(powers, axis=0).astype(BF16)
            product = jnp.dot(weights, values, preferred_element_type=F32)
            top = jnp.zeros((HALF, 128), F32)
            bottom = jnp.zeros((HALF, 128), F32)
            for h in range(GROUP):
                part = product[h * HALF : (h + 1) * HALF]
                top = jnp.where(lane_head == h, part[:, :128], top)
                bottom = jnp.where(lane_head == h, part[:, 128:], bottom)
            out.append(top / bottom)
        return jnp.concatenate(out, axis=1)

    for c in copies1 + copiese:
        c.wait_recv()
    other = jnp.concatenate([ref[...].reshape(-1, features) for ref in (halo1, haloe)], axis=0)
    full = rounded(jnp.dot(other, w_qkv[:, WIDTH:], preferred_element_type=F32))
    for c in range(2):
        for rh in range(2):
            put_piece(3 * c, full[(2 * rh + c) * HALF : (2 * rh + c + 1) * HALF], rh)

    def edge_unit(half, carry):
        for a in range(2):
            result = attend(a, 1, half)
            for k in range(2):
                place = (2 * a + k + 1) % 4 * PIECE
                att1[half, place : place + PIECE, :] = result[2 * k * PIECE : (2 * k + 1) * PIECE]
                atte[half, place : place + PIECE, :] = result[(2 * k + 1) * PIECE : (2 * k + 2) * PIECE]
        return carry

    lax.fori_loop(0, 2, edge_unit, 0)
    atte_out[...] = atte[...].astype(BF16)
    return_copy = remote(atte_out, atte_in, lat_send.at[1], lat_recv.at[1], partner)
    return_copy.start()

    for c in copies0:
        c.wait_recv()
    full = rounded(jnp.dot(halo0[...].reshape(-1, features), w_qkv[:, WIDTH:], preferred_element_type=F32))
    for c in range(2):
        put_main(3 * c, full[c * 2 * HALF : (c + 1) * 2 * HALF])

    def main_unit(half, carry):
        for a in range(2):
            result = attend(a, 0, half)
            for k in range(2):
                place = (2 * a + k + 1) % 4 * 2 * PIECE
                att0[half, place : place + 2 * PIECE, :] = result[k * 2 * PIECE : (k + 1) * 2 * PIECE]
        return carry

    lax.fori_loop(0, 2, main_unit, 0)
    for load in loads[5:]:
        load.wait()

    def finish(attended, hidden):
        projected = jnp.dot(attended.astype(BF16), w_proj[...], preferred_element_type=F32) + proj_bias_ref[...][None]
        average = jnp.mean(projected, axis=-1, keepdims=True)
        centered = projected - average
        spread = jnp.mean(centered * centered, axis=-1, keepdims=True)
        normed = centered * lax.rsqrt(spread + norm_epsilon) * gain_ref[...][None] + shift_ref[...][None]
        return hidden.astype(F32) + normed

    def keep(half, start, values):
        for k in range(tokens.shape[1]):
            tokens[half, k, start : start + values.shape[0], :] = values[:, k * 128 : (k + 1) * 128]

    def emit(row_range):
        for r in row_range:
            for half in range(2):
                for c in range(6):
                    place, step = place_of(r, half, c)
                    found = [tokens[half, k, pl.ds(place, levels, stride=step), :] for k in range(tokens.shape[1])]
                    out_ref[r, half * 6 + c] = jnp.concatenate(found, axis=1).astype(BF16)

    for half in range(2):
        keep(half, 0, finish(att0[half], m0_ref[half]))
        keep(half, 8 * PIECE, finish(att1[half], m1_ref[half]))
    emit(range(3, 12))
    stores = [
        pltpu.make_async_copy(out_ref.at[pl.ds(first, size)], out_hbm.at[pl.ds(first, size)], out_sem.at[k])
        for k, (first, size) in enumerate([(3, 9), (0, 3)])
    ]
    stores[0].start()
    return_copy.wait_recv()
    for half in range(2):
        keep(half, 12 * PIECE, finish(atte_in[half], ed_ref[half]))
    emit(range(3))
    stores[1].start()
    edge_copy.wait_send()
    return_copy.wait_send()
    for c in copies1 + copiese + copies0:
        c.wait_send()
    for store in stores:
        store.wait()


def on_device(
    state_tokens,
    land_mask,
    pad_mask,
    land_embed,
    w_qkv,
    w_proj,
    proj_bias,
    norm_gain,
    norm_shift,
    bias_table,
    index_table,
):
    levels, lat_rows, lon_columns, features = state_tokens.shape
    lat_windows, z_windows, heads, positions = bias_table.shape
    lat_total = lat_rows * lax.axis_size("lat")
    half_columns = WIN_LON // 2
    blocks = -(-positions // SPAN)

    side = (2, levels * PIECE, features)
    main = (2, levels * 2 * PIECE, features)
    rows = z_windows * lat_windows * heads

    state = state_tokens.transpose(1, 2, 0, 3)
    tables = bias_table.transpose(0, 2, 1, 3)
    anywhere = pl.BlockSpec(memory_space=pl.ANY)
    smem = pl.BlockSpec(memory_space=pltpu.SMEM)
    result = pl.pallas_call(
        functools.partial(kernel, lat_total, blocks),
        out_shape=jax.ShapeDtypeStruct(state.shape, BF16),
        in_specs=[anywhere] * 9 + [smem] * 2,
        out_specs=anywhere,
        scratch_shapes=[
            pltpu.VMEM(state.shape, BF16),
            pltpu.VMEM(land_embed.shape, F32),
            pltpu.VMEM(index_table.shape, jnp.int32),
            pltpu.VMEM(tables.shape, BF16),
            pltpu.VMEM(proj_bias.shape, F32),
            pltpu.VMEM(norm_gain.shape, F32),
            pltpu.VMEM(norm_shift.shape, F32),
            pltpu.VMEM(state.shape, BF16),
            pltpu.VMEM((2, features // 128, 16 * PIECE, 128), F32),
            pltpu.VMEM(main, BF16),
            pltpu.VMEM(side, BF16),
            pltpu.VMEM(side, BF16),
            pltpu.VMEM((2, blocks * rows, 128), F32),
            pltpu.VMEM((blocks * rows, SPAN), BF16),
            pltpu.VMEM((WIN_TOK, WIN_TOK), jnp.int32),
            pltpu.VMEM((WIN_TOK // T_STEP, T_STEP * WIN_TOK), jnp.int32),
            pltpu.VMEM(w_qkv.shape, BF16),
            pltpu.VMEM(w_proj.shape, BF16),
            pltpu.VMEM(side, BF16),
            pltpu.VMEM(main, BF16),
            pltpu.VMEM(side, BF16),
            pltpu.VMEM(side, BF16),
            pltpu.VMEM((2, 2, 2, HALF, WIDTH), F32),
            pltpu.VMEM((4, 2, 2, HALF, 2 * WIDTH), F32),
            pltpu.VMEM((rows, T_STEP * WIN_TOK + 128), F32),
            pltpu.VMEM((2, rows * WIN_TOK, 128), F32),
            pltpu.VMEM((2, 2 * HALF, WIDTH), F32),
            pltpu.VMEM((2, HALF, WIDTH), F32),
            pltpu.VMEM((2, HALF, WIDTH), F32),
            pltpu.VMEM((2, HALF, WIDTH), BF16),
            pltpu.VMEM((2, HALF, WIDTH), BF16),
            pltpu.SemaphoreType.DMA((9,)),
            pltpu.SemaphoreType.DMA((2,)),
            pltpu.SemaphoreType.DMA((2,)),
            pltpu.SemaphoreType.DMA((2,)),
            pltpu.SemaphoreType.DMA((6,)),
            pltpu.SemaphoreType.DMA((6,)),
        ],
        compiler_params=pltpu.CompilerParams(
            collective_id=0, has_side_effects=True, vmem_limit_bytes=56 * 1024 * 1024
        ),
        name="window_layer",
    )(
        state,
        land_embed,
        index_table,
        tables,
        w_qkv,
        w_proj,
        proj_bias,
        norm_gain,
        norm_shift,
        land_mask,
        pad_mask,
    )
    return result.transpose(2, 0, 1, 3)


def solution(mesh):
    in_specs = (
        P("member", "lat", "lon", None),
        P("lat", "lon"),
        P(),
        P(),
        P(),
        P(),
        P(),
        P(),
        P(),
        P("lat", None, None, None),
        P(),
    )
    out_specs = P("member", "lat", "lon", None)
    return jax.shard_map(
        on_device, mesh=mesh, in_specs=in_specs, out_specs=out_specs, check_vma=False
    )
```

```python
import functools

import jax
import jax.numpy as jnp
from jax import lax
from jax.experimental import pallas as pl
from jax.experimental.pallas import tpu as pltpu
from jax.sharding import PartitionSpec as P

HEADS = 12
HEAD_DIM = 32
WIDTH = HEADS * HEAD_DIM
WIN_Z = 2
WIN_LAT = 6
WIN_LON = 12
WIN_TOK = 144
HALF = 72
PIECE = 18
GROUP = 4
GROUPS = HEADS // GROUP
UNROLL = 9
T_STEP = 16
SPAN = 256
NEG = -1e30

norm_epsilon = 1e-05

MESH = pl.DeviceIdType.MESH
F32 = jnp.float32
BF16 = jnp.bfloat16


def nt_dot(a, b):
    return lax.dot_general(a, b, (((1,), (1,)), ((), ())), preferred_element_type=F32)


def kernel(
    lat_total,
    blocks,
    state_hbm,
    embed_hbm,
    index_hbm,
    bias_table_hbm,
    w_qkv_hbm,
    w_proj_hbm,
    proj_bias_hbm,
    gain_hbm,
    shift_hbm,
    land_ref,
    pad_ref,
    out_hbm,
    state_ref,
    embed_ref,
    index_ref,
    bias_table_ref,
    proj_bias_ref,
    gain_ref,
    shift_ref,
    out_ref,
    tokens,
    m0_ref,
    m1_ref,
    ed_ref,
    table32,
    table_ref,
    ordered,
    masks,
    idx_ref,
    w_qkv,
    w_proj,
    edge_in,
    halo0,
    halo1,
    haloe,
    q_buf,
    kv_buf,
    acc,
    bias,
    att0,
    att1,
    atte,
    atte_out,
    atte_in,
    w_sem,
    out_sem,
    lat_send,
    lat_recv,
    lon_send,
    lon_recv,
):
    member = lax.axis_index("member")
    lon = lax.axis_index("lon")
    lat = lax.axis_index("lat")
    lon_size = lax.axis_size("lon")
    left = (member, lax.rem(lon + lon_size - 1, lon_size), lat)
    right = (member, lax.rem(lon + 1, lon_size), lat)
    partner = (member, lon, 1 - lat)

    barrier = pltpu.get_barrier_semaphore()
    for other in (left, right, partner):
        pl.semaphore_signal(barrier, inc=1, device_id=other, device_id_type=MESH)

    loads = [
        pltpu.make_async_copy(src, dst, w_sem.at[k])
        for k, (src, dst) in enumerate(
            [
                (embed_hbm, embed_ref),
                (state_hbm, state_ref),
                (index_hbm, index_ref),
                (bias_table_hbm, bias_table_ref),
                (w_qkv_hbm, w_qkv),
                (w_proj_hbm, w_proj),
                (proj_bias_hbm, proj_bias_ref),
                (gain_hbm, gain_ref),
                (shift_hbm, shift_ref),
            ]
        )
    ]
    for load in loads[:2]:
        load.start()

    levels = state_ref.shape[2]

    def place_of(r, half, c):
        if r < 3:
            return 12 * PIECE + r * 6 + c, PIECE
        if r < 9:
            return (r - 3) * 6 + c, 2 * PIECE
        return 8 * PIECE + (r - 9) * 6 + c, PIECE

    loads[0].wait()
    loads[1].wait()
    for load in loads[2:]:
        load.start()
    sea = jnp.broadcast_to(embed_ref[0:1, :], (levels, embed_ref.shape[1]))
    ground = jnp.broadcast_to(embed_ref[1:2, :], (levels, embed_ref.shape[1]))

    def prepare(row_range):
        for r in row_range:
            for half in range(2):
                for c in range(6):
                    column = half * 6 + c
                    embedded = jnp.where(land_ref[r, column] == 1, ground, sea)
                    full = state_ref[r, column].astype(F32) + embedded
                    place, step = place_of(r, half, c)
                    for k in range(0, full.shape[1], 128):
                        tokens[half, k // 128, pl.ds(place, levels, stride=step), :] = full[:, k : k + 128]

    def joined(half, start, stop):
        return jnp.concatenate([tokens[half, k, start:stop, :] for k in range(tokens.shape[1])], axis=1)

    def gathered(ref, start, stop):
        for half in range(2):
            ref[half] = joined(half, start, stop).astype(BF16)

    prepare(range(3))
    gathered(ed_ref, 12 * PIECE, 16 * PIECE)
    prepare(range(9, 12))
    gathered(m1_ref, 8 * PIECE, 12 * PIECE)
    pl.semaphore_wait(barrier, 3)

    def remote(src, dst, send, recv, to):
        return pltpu.make_async_remote_copy(
            src_ref=src, dst_ref=dst, send_sem=send, recv_sem=recv, device_id=to, device_id_type=MESH
        )

    edge_copy = remote(ed_ref, edge_in, lat_send.at[0], lat_recv.at[0], partner)
    edge_copy.start()

    def lon_copies(own, halo, k):
        return [
            remote(own.at[0], halo.at[1], lon_send.at[2 * k], lon_recv.at[2 * k], left),
            remote(own.at[1], halo.at[0], lon_send.at[2 * k + 1], lon_recv.at[2 * k + 1], right),
        ]

    copies1 = lon_copies(m1_ref, halo1, 0)
    copiese = lon_copies(edge_in, haloe, 1)
    copies0 = lon_copies(m0_ref, halo0, 2)
    for c in copies1:
        c.start()

    prepare(range(3, 9))
    gathered(m0_ref, 0, 8 * PIECE)

    part_rows = table_ref.shape[0] // 2
    tables = 2 * HEADS
    positions = bias_table_ref.shape[3]
    loads[3].wait()
    spare = jnp.zeros((part_rows - blocks * tables, 128), F32)
    for k in range(2):
        for z in range(2):
            table32[k, z * part_rows + blocks * tables : (z + 1) * part_rows, :] = spare
    for b in range(2):
        for h in range(HEADS):
            both = bias_table_ref[b, h].astype(F32)
            for k in range(blocks * SPAN // 128):
                place = k // 2 * tables + b * HEADS + h
                stop = min(positions, (k + 1) * 128)
                part = both[:, k * 128 : stop]
                if stop < (k + 1) * 128:
                    part = jnp.concatenate([part, jnp.zeros((2, (k + 1) * 128 - stop), F32)], axis=1)
                table32[k % 2, pl.ds(place, 2, stride=part_rows), :] = part
    table_ref[...] = jnp.concatenate([table32[0], table32[1]], axis=1).astype(BF16)

    new = lax.broadcasted_iota(jnp.int32, (WIN_TOK, WIN_TOK), 0)
    old = lax.broadcasted_iota(jnp.int32, (WIN_TOK, WIN_TOK), 1)
    inside = new % HALF
    quarter = HALF // 2

    def chosen(place):
        return jnp.where(old == place, 1.0, 0.0).astype(BF16)

    query_order = chosen(inside // 6 * WIN_LON + new // HALF * 6 + inside % 6)
    key_order = chosen(new // HALF * HALF + inside % quarter // 6 * WIN_LON + inside // quarter * 6 + inside % 6)

    def reorder(x):
        x = jnp.dot(query_order, x.astype(F32).astype(BF16), preferred_element_type=F32)
        return nt_dot(x.astype(BF16), key_order)

    loads[2].wait()
    index = index_ref[...]
    index = (reorder(index >> 8) * SPAN + reorder(index & (SPAN - 1))).astype(jnp.int32)
    lower = lax.broadcasted_iota(jnp.int32, (WIN_TOK, HALF), 0) % HALF < quarter
    ordered[0] = jnp.where(lower, index[:, :HALF], index[:, HALF:])
    ordered[1] = jnp.where(lower, index[:, HALF:], index[:, :HALF])
    steps = WIN_TOK // T_STEP
    spread = T_STEP * HALF
    for i in range(T_STEP):
        for other in range(2):
            start = other * spread + i * HALF
            idx_ref[:, start : start + HALF] = ordered[other, i * steps : (i + 1) * steps, :]

    lane = lax.broadcasted_iota(jnp.int32, (HALF, 128), 1)
    row = lax.broadcasted_iota(jnp.int32, (HALF, 128), 0)
    lane_head = lane // HEAD_DIM
    lat_start = lat * 2 * WIN_LAT
    same_level = (lane // quarter) == (row // quarter)
    same_rows = (lane // PIECE) % 2 == (row // PIECE) % 2
    lane_row = lane % quarter // WIN_LAT
    for b in range(2):
        wraps = lat_start + b * WIN_LAT >= lat_total - WIN_LAT
        usable = jnp.zeros((HALF, 128), jnp.int32)
        for r in range(WIN_LAT):
            value = pad_ref[lax.rem(lat_start + b * WIN_LAT + r + WIN_LAT // 2, lat_total)]
            usable = jnp.where(lane_row == r, value, usable)
        allowed = (lane < HALF) & (usable == 1) & jnp.logical_or(jnp.logical_not(wraps), same_rows)
        masks[0, b] = jnp.where(allowed, 1, 0)
        masks[1, b] = jnp.where(allowed & same_level, 1, 0)

    first_part = lax.broadcasted_iota(jnp.int32, (tables, 128), 1) < quarter
    width = 2 * spread

    def bias_step(outer, carry):
        for inner in range(UNROLL):
            bias_rows(outer * UNROLL + inner, acc.at[inner])
        return carry

    def bias_rows(step, acc):
        def find(j):
            lanes = slice(j * 256, (j + 1) * 256)
            both = j * 256 < spread
            picked = idx_ref[pl.ds(step, 1), lanes]
            low = jnp.broadcast_to(picked & (SPAN - 1), (SPAN, 256))
            hot = jnp.where(lax.broadcasted_iota(jnp.int32, (SPAN, 256), 0) == low, 1.0, 0.0).astype(BF16)
            high = jnp.broadcast_to(picked >> 8, (tables, 256))
            entries = table_ref[...] if both else table_ref[:part_rows]
            found = jnp.dot(entries, hot, preferred_element_type=F32)
            for z in range(2 if both else 1):
                start = z * part_rows
                total = found[start : start + tables]
                for k in range(1, blocks):
                    total = jnp.where(high == k, found[start + k * tables : start + (k + 1) * tables], total)
                acc[z, :, lanes] = total

        def moved(z, source, target):
            base = source // 128 * 128
            shift = target - (source - base)
            if source - base + quarter <= 128:
                piece = acc[z, :, base : base + 128]
                return pltpu.roll(piece, shift % 128, 1) if shift % 128 else piece
            return pltpu.roll(acc[z, :, base : base + 256], shift % 256, 1)[:, :128]

        def keep_row(i):
            level = i // (T_STEP // 4) % 2
            for c in range(2):
                near = i * HALF + c * quarter
                same = moved(0, near, level * quarter)
                cross = moved(0, spread + near, (1 - level) * quarter)
                pair = (same, cross) if level == 0 else (cross, same)
                place = i * steps + step
                bias[c, pl.ds(place, tables, stride=WIN_TOK), :] = jnp.where(first_part, *pair)
                bias[c, pl.ds(tables * WIN_TOK + place, tables, stride=WIN_TOK), :] = moved(1, near, level * quarter)

        done = set()
        kept = 0
        for j in (0, 4, 5, 1, 6, 2, 7, 3, 8):
            find(j)
            done.add(j)
            while kept < T_STEP and all(
                p // 256 in done
                for start in (kept * HALF, spread + kept * HALF)
                for p in range(start, start + HALF)
            ):
                keep_row(kept)
                kept += 1

    edge_copy.wait_recv()
    for c in copiese:
        c.start()
    for c in copies0:
        c.start()

    lax.fori_loop(0, steps // UNROLL, bias_step, 0)

    loads[4].wait()

    def rounded(x):
        return x.astype(BF16).astype(F32)

    def put_main(slot, both):
        for level in range(4):
            rolled = (level + 3) % 4
            start = (rolled % 2) * 2 * PIECE
            kv_buf[slot, rolled // 2, 0, start : start + 2 * PIECE, :] = both[
                level * 2 * PIECE : (level + 1) * 2 * PIECE
            ]

    def put_piece(slot, both, rh):
        for level in range(4):
            rolled = (level + 3) % 4
            start = (rolled % 2) * 2 * PIECE + rh * PIECE
            kv_buf[slot, rolled // 2, 1, start : start + PIECE, :] = both[level * PIECE : (level + 1) * PIECE]

    def put_query_main(half, both):
        for level in range(4):
            rolled = (level + 3) % 4
            start = (rolled % 2) * 2 * PIECE
            q_buf[half, rolled // 2, 0, start : start + 2 * PIECE, :] = both[
                level * 2 * PIECE : (level + 1) * 2 * PIECE
            ]

    def put_query(half, both, rh):
        for level in range(4):
            rolled = (level + 3) % 4
            start = (rolled % 2) * 2 * PIECE + rh * PIECE
            q_buf[half, rolled // 2, 1, start : start + PIECE, :] = both[level * PIECE : (level + 1) * PIECE]

    features = w_qkv.shape[0]
    own = jnp.concatenate(
        [ref[...].reshape(-1, features) for ref in (m0_ref, m1_ref, edge_in)], axis=0
    )
    full = rounded(jnp.dot(own, w_qkv[...], preferred_element_type=F32))
    for half in range(2):
        main = full[half * 2 * HALF : (half + 1) * 2 * HALF]
        put_query_main(half, main[:, :WIDTH])
        put_main(half + 1, main[:, WIDTH:])
        for rh in range(2):
            part = full[(4 + 2 * rh + half) * HALF : (5 + 2 * rh + half) * HALF]
            put_query(half, part[:, :WIDTH], rh)
            put_piece(half + 1, part[:, WIDTH:], rh)

    def attend(a, b, half):
        allowed = masks[a, b] == 1
        slot0 = 2 * half
        out = []
        zeros = jnp.zeros((128 - HALF, 128), F32)
        ones = jnp.ones((256, 128), BF16)
        query_half = 1 - half
        for g in range(GROUPS):
            cols = slice(g * 128, (g + 1) * 128)
            vcols = slice(WIDTH + g * 128, WIDTH + (g + 1) * 128)
            q = q_buf[half, a, b, :, cols]
            stacked = jnp.concatenate([jnp.where(lane_head == h, q, 0.0) for h in range(GROUP)], axis=0).astype(BF16)
            keys = jnp.concatenate(
                [kv_buf[slot0, a, b, :, cols], zeros, kv_buf[slot0 + 1, a, b, :, cols], zeros], axis=0
            ).astype(BF16)
            values = jnp.concatenate(
                [kv_buf[slot0, a, b, :, vcols], zeros, kv_buf[slot0 + 1, a, b, :, vcols], zeros], axis=0
            ).astype(BF16)
            values = jnp.concatenate([values, ones], axis=1)
            scores = nt_dot(stacked, keys)
            powers = []
            for h in range(GROUP):
                first = ((a * 2 + b) * HEADS + g * GROUP + h) * WIN_TOK + query_half * HALF
                parts = []
                for c in range(2):
                    s = scores[h * HALF : (h + 1) * HALF, c * 128 : (c + 1) * 128] * (HEAD_DIM**-0.5)
                    s = s + bias[c, pl.ds(pl.multiple_of(first, 8), HALF), :]
                    parts.append(jnp.where(allowed, s, NEG))
                largest = jnp.max(jnp.maximum(parts[0], parts[1]), axis=1, keepdims=True)
                powers.append(jnp.concatenate([jnp.exp(p - largest) for p in parts], axis=1))
            weights = jnp.concatenate(powers, axis=0).astype(BF16)
            product = jnp.dot(weights, values, preferred_element_type=F32)
            top = jnp.zeros((HALF, 128), F32)
            bottom = jnp.zeros((HALF, 128), F32)
            for h in range(GROUP):
                part = product[h * HALF : (h + 1) * HALF]
                top = jnp.where(lane_head == h, part[:, :128], top)
                bottom = jnp.where(lane_head == h, part[:, 128:], bottom)
            out.append(top / bottom)
        return jnp.concatenate(out, axis=1)

    for c in copies1 + copiese:
        c.wait_recv()
    other = jnp.concatenate([ref[...].reshape(-1, features) for ref in (halo1, haloe)], axis=0)
    full = rounded(jnp.dot(other, w_qkv[:, WIDTH:], preferred_element_type=F32))
    for c in range(2):
        for rh in range(2):
            put_piece(3 * c, full[(2 * rh + c) * HALF : (2 * rh + c + 1) * HALF], rh)

    def edge_unit(half, carry):
        for a in range(2):
            result = attend(a, 1, half)
            for k in range(2):
                place = (2 * a + k + 1) % 4 * PIECE
                att1[half, place : place + PIECE, :] = result[2 * k * PIECE : (2 * k + 1) * PIECE]
                atte[half, place : place + PIECE, :] = result[(2 * k + 1) * PIECE : (2 * k + 2) * PIECE]
        return carry

    lax.fori_loop(0, 2, edge_unit, 0)
    atte_out[...] = atte[...].astype(BF16)
    return_copy = remote(atte_out, atte_in, lat_send.at[1], lat_recv.at[1], partner)
    return_copy.start()

    for c in copies0:
        c.wait_recv()
    full = rounded(jnp.dot(halo0[...].reshape(-1, features), w_qkv[:, WIDTH:], preferred_element_type=F32))
    for c in range(2):
        put_main(3 * c, full[c * 2 * HALF : (c + 1) * 2 * HALF])

    def main_unit(half, carry):
        for a in range(2):
            result = attend(a, 0, half)
            for k in range(2):
                place = (2 * a + k + 1) % 4 * 2 * PIECE
                att0[half, place : place + 2 * PIECE, :] = result[k * 2 * PIECE : (k + 1) * 2 * PIECE]
        return carry

    lax.fori_loop(0, 2, main_unit, 0)
    for load in loads[5:]:
        load.wait()

    def finish(attended, hidden):
        projected = jnp.dot(attended.astype(BF16), w_proj[...], preferred_element_type=F32) + proj_bias_ref[...][None]
        average = jnp.mean(projected, axis=-1, keepdims=True)
        centered = projected - average
        spread = jnp.mean(centered * centered, axis=-1, keepdims=True)
        normed = centered * lax.rsqrt(spread + norm_epsilon) * gain_ref[...][None] + shift_ref[...][None]
        return hidden.astype(F32) + normed

    def keep(half, start, values):
        for k in range(tokens.shape[1]):
            tokens[half, k, start : start + values.shape[0], :] = values[:, k * 128 : (k + 1) * 128]

    def emit(row_range):
        for r in row_range:
            for half in range(2):
                for c in range(6):
                    place, step = place_of(r, half, c)
                    found = [tokens[half, k, pl.ds(place, levels, stride=step), :] for k in range(tokens.shape[1])]
                    out_ref[r, half * 6 + c] = jnp.concatenate(found, axis=1).astype(BF16)

    for half in range(2):
        keep(half, 0, finish(att0[half], m0_ref[half]))
        keep(half, 8 * PIECE, finish(att1[half], m1_ref[half]))
    emit(range(3, 12))
    stores = [
        pltpu.make_async_copy(out_ref.at[pl.ds(first, size)], out_hbm.at[pl.ds(first, size)], out_sem.at[k])
        for k, (first, size) in enumerate([(3, 9), (0, 3)])
    ]
    stores[0].start()
    return_copy.wait_recv()
    for half in range(2):
        keep(half, 12 * PIECE, finish(atte_in[half], ed_ref[half]))
    emit(range(3))
    stores[1].start()
    edge_copy.wait_send()
    return_copy.wait_send()
    for c in copies1 + copiese + copies0:
        c.wait_send()
    for store in stores:
        store.wait()


def on_device(
    state_tokens,
    land_mask,
    pad_mask,
    land_embed,
    w_qkv,
    w_proj,
    proj_bias,
    norm_gain,
    norm_shift,
    bias_table,
    index_table,
):
    levels, lat_rows, lon_columns, features = state_tokens.shape
    lat_windows, z_windows, heads, positions = bias_table.shape
    lat_total = lat_rows * lax.axis_size("lat")
    half_columns = WIN_LON // 2
    blocks = -(-positions // SPAN)

    side = (2, levels * PIECE, features)
    main = (2, levels * 2 * PIECE, features)
    rows = z_windows * lat_windows * heads
    table_rows = -(-blocks * lat_windows * heads // 16) * 16

    state = state_tokens.transpose(1, 2, 0, 3)
    tables = bias_table.transpose(0, 2, 1, 3)
    anywhere = pl.BlockSpec(memory_space=pl.ANY)
    smem = pl.BlockSpec(memory_space=pltpu.SMEM)
    result = pl.pallas_call(
        functools.partial(kernel, lat_total, blocks),
        out_shape=jax.ShapeDtypeStruct(state.shape, BF16),
        in_specs=[anywhere] * 9 + [smem] * 2,
        out_specs=anywhere,
        scratch_shapes=[
            pltpu.VMEM(state.shape, BF16),
            pltpu.VMEM(land_embed.shape, F32),
            pltpu.VMEM(index_table.shape, jnp.int32),
            pltpu.VMEM(tables.shape, BF16),
            pltpu.VMEM(proj_bias.shape, F32),
            pltpu.VMEM(norm_gain.shape, F32),
            pltpu.VMEM(norm_shift.shape, F32),
            pltpu.VMEM(state.shape, BF16),
            pltpu.VMEM((2, features // 128, 16 * PIECE, 128), F32),
            pltpu.VMEM(main, BF16),
            pltpu.VMEM(side, BF16),
            pltpu.VMEM(side, BF16),
            pltpu.VMEM((2, z_windows * table_rows, 128), F32),
            pltpu.VMEM((z_windows * table_rows, SPAN), BF16),
            pltpu.VMEM((2, WIN_TOK, HALF), jnp.int32),
            pltpu.VMEM((2, 2, HALF, 128), jnp.int32),
            pltpu.VMEM((WIN_TOK // T_STEP, T_STEP * WIN_TOK), jnp.int32),
            pltpu.VMEM(w_qkv.shape, BF16),
            pltpu.VMEM(w_proj.shape, BF16),
            pltpu.VMEM(side, BF16),
            pltpu.VMEM(main, BF16),
            pltpu.VMEM(side, BF16),
            pltpu.VMEM(side, BF16),
            pltpu.VMEM((2, 2, 2, HALF, WIDTH), F32),
            pltpu.VMEM((4, 2, 2, HALF, 2 * WIDTH), F32),
            pltpu.VMEM((UNROLL, 2, lat_windows * heads, T_STEP * WIN_TOK + 128), F32),
            pltpu.VMEM((2, rows * WIN_TOK, 128), F32),
            pltpu.VMEM((2, 2 * HALF, WIDTH), F32),
            pltpu.VMEM((2, HALF, WIDTH), F32),
            pltpu.VMEM((2, HALF, WIDTH), F32),
            pltpu.VMEM((2, HALF, WIDTH), BF16),
            pltpu.VMEM((2, HALF, WIDTH), BF16),
            pltpu.SemaphoreType.DMA((9,)),
            pltpu.SemaphoreType.DMA((2,)),
            pltpu.SemaphoreType.DMA((2,)),
            pltpu.SemaphoreType.DMA((2,)),
            pltpu.SemaphoreType.DMA((6,)),
            pltpu.SemaphoreType.DMA((6,)),
        ],
        compiler_params=pltpu.CompilerParams(
            collective_id=0, has_side_effects=True, vmem_limit_bytes=56 * 1024 * 1024
        ),
        name="window_layer",
    )(
        state,
        land_embed,
        index_table,
        tables,
        w_qkv,
        w_proj,
        proj_bias,
        norm_gain,
        norm_shift,
        land_mask,
        pad_mask,
    )
    return result.transpose(2, 0, 1, 3)


def solution(mesh):
    in_specs = (
        P("member", "lat", "lon", None),
        P("lat", "lon"),
        P(),
        P(),
        P(),
        P(),
        P(),
        P(),
        P(),
        P("lat", None, None, None),
        P(),
    )
    out_specs = P("member", "lat", "lon", None)
    return jax.shard_map(
        on_device, mesh=mesh, in_specs=in_specs, out_specs=out_specs, check_vma=False
    )
```

```python
import functools

import jax
import jax.numpy as jnp
from jax import lax
from jax.experimental import pallas as pl
from jax.experimental.pallas import tpu as pltpu
from jax.sharding import PartitionSpec as P

HEADS = 12
HEAD_DIM = 32
WIDTH = HEADS * HEAD_DIM
WIN_Z = 2
WIN_LAT = 6
WIN_LON = 12
WIN_TOK = 144
HALF = 72
PIECE = 18
GROUP = 4
GROUPS = HEADS // GROUP
NORM_ROWS = 48
T_STEP = 16
SPAN = 256
NEG = -1e30

norm_epsilon = 1e-05

MESH = pl.DeviceIdType.MESH
F32 = jnp.float32
BF16 = jnp.bfloat16


def nt_dot(a, b):
    return lax.dot_general(a, b, (((1,), (1,)), ((), ())), preferred_element_type=F32)


def kernel(
    lat_total,
    blocks,
    state_hbm,
    embed_hbm,
    index_hbm,
    bias_table_hbm,
    w_qkv_hbm,
    w_proj_hbm,
    proj_bias_hbm,
    gain_hbm,
    shift_hbm,
    land_ref,
    pad_ref,
    out_hbm,
    state_ref,
    embed_ref,
    index_ref,
    bias_table_ref,
    proj_bias_ref,
    gain_ref,
    shift_ref,
    out_ref,
    tokens,
    m0_ref,
    m1_ref,
    ed_ref,
    table32,
    table_ref,
    ordered,
    masks,
    idx_ref,
    w_qkv,
    w_proj,
    edge_in,
    halo0,
    halo1,
    haloe,
    q_buf,
    kv_buf,
    acc,
    bias,
    att0,
    att1,
    atte,
    atte_out,
    atte_in,
    w_sem,
    out_sem,
    lat_send,
    lat_recv,
    lon_send,
    lon_recv,
):
    member = lax.axis_index("member")
    lon = lax.axis_index("lon")
    lat = lax.axis_index("lat")
    lon_size = lax.axis_size("lon")
    left = (member, lax.rem(lon + lon_size - 1, lon_size), lat)
    right = (member, lax.rem(lon + 1, lon_size), lat)
    partner = (member, lon, 1 - lat)

    barrier = pltpu.get_barrier_semaphore()
    for other in (left, right, partner):
        pl.semaphore_signal(barrier, inc=1, device_id=other, device_id_type=MESH)

    loads = [
        pltpu.make_async_copy(src, dst, w_sem.at[k])
        for k, (src, dst) in enumerate(
            [
                (embed_hbm, embed_ref),
                (state_hbm, state_ref),
                (index_hbm, index_ref),
                (bias_table_hbm, bias_table_ref),
                (w_qkv_hbm, w_qkv),
                (w_proj_hbm, w_proj),
                (proj_bias_hbm, proj_bias_ref),
                (gain_hbm, gain_ref),
                (shift_hbm, shift_ref),
            ]
        )
    ]
    for load in loads[:2]:
        load.start()

    levels = state_ref.shape[2]

    def place_of(r, half, c):
        if r < 3:
            return 12 * PIECE + r * 6 + c, PIECE
        if r < 9:
            return (r - 3) * 6 + c, 2 * PIECE
        return 8 * PIECE + (r - 9) * 6 + c, PIECE

    loads[0].wait()
    loads[1].wait()
    for load in loads[2:]:
        load.start()
    sea = jnp.broadcast_to(embed_ref[0:1, :], (levels, embed_ref.shape[1]))
    ground = jnp.broadcast_to(embed_ref[1:2, :], (levels, embed_ref.shape[1]))

    def prepare(row_range):
        for r in row_range:
            for half in range(2):
                for c in range(6):
                    column = half * 6 + c
                    embedded = jnp.where(land_ref[r, column] == 1, ground, sea)
                    full = state_ref[r, column].astype(F32) + embedded
                    place, step = place_of(r, half, c)
                    for k in range(0, full.shape[1], 128):
                        tokens[half, k // 128, pl.ds(place, levels, stride=step), :] = full[:, k : k + 128]

    def joined(half, start, stop):
        return jnp.concatenate([tokens[half, k, start:stop, :] for k in range(tokens.shape[1])], axis=1)

    def gathered(ref, start, stop):
        for half in range(2):
            ref[half] = joined(half, start, stop).astype(BF16)

    prepare(range(3))
    gathered(ed_ref, 12 * PIECE, 16 * PIECE)
    prepare(range(9, 12))
    gathered(m1_ref, 8 * PIECE, 12 * PIECE)
    pl.semaphore_wait(barrier, 3)

    def remote(src, dst, send, recv, to):
        return pltpu.make_async_remote_copy(
            src_ref=src, dst_ref=dst, send_sem=send, recv_sem=recv, device_id=to, device_id_type=MESH
        )

    edge_copy = remote(ed_ref, edge_in, lat_send.at[0], lat_recv.at[0], partner)
    edge_copy.start()

    def lon_copies(own, halo, k):
        return [
            remote(own.at[0], halo.at[1], lon_send.at[2 * k], lon_recv.at[2 * k], left),
            remote(own.at[1], halo.at[0], lon_send.at[2 * k + 1], lon_recv.at[2 * k + 1], right),
        ]

    copies1 = lon_copies(m1_ref, halo1, 0)
    copiese = lon_copies(edge_in, haloe, 1)
    copies0 = lon_copies(m0_ref, halo0, 2)
    for c in copies1:
        c.start()

    prepare(range(3, 9))
    gathered(m0_ref, 0, 8 * PIECE)

    part_rows = table_ref.shape[0] // 2
    tables = 2 * HEADS
    positions = bias_table_ref.shape[3]
    loads[3].wait()
    spare = jnp.zeros((part_rows - blocks * tables, 128), F32)
    for k in range(2):
        for z in range(2):
            table32[k, z * part_rows + blocks * tables : (z + 1) * part_rows, :] = spare
    for b in range(2):
        for h in range(HEADS):
            both = bias_table_ref[b, h].astype(F32)
            for k in range(blocks * SPAN // 128):
                place = k // 2 * tables + b * HEADS + h
                stop = min(positions, (k + 1) * 128)
                part = both[:, k * 128 : stop]
                if stop < (k + 1) * 128:
                    part = jnp.concatenate([part, jnp.zeros((2, (k + 1) * 128 - stop), F32)], axis=1)
                table32[k % 2, pl.ds(place, 2, stride=part_rows), :] = part
    table_ref[...] = jnp.concatenate([table32[0], table32[1]], axis=1).astype(BF16)

    new = lax.broadcasted_iota(jnp.int32, (WIN_TOK, WIN_TOK), 0)
    old = lax.broadcasted_iota(jnp.int32, (WIN_TOK, WIN_TOK), 1)
    inside = new % HALF
    quarter = HALF // 2

    def chosen(place):
        return jnp.where(old == place, 1.0, 0.0).astype(BF16)

    query_order = chosen(inside // 6 * WIN_LON + new // HALF * 6 + inside % 6)
    key_order = chosen(new // HALF * HALF + inside % quarter // 6 * WIN_LON + inside // quarter * 6 + inside % 6)

    def reorder(x):
        x = jnp.dot(query_order, x.astype(F32).astype(BF16), preferred_element_type=F32)
        return nt_dot(x.astype(BF16), key_order)

    loads[2].wait()
    index = index_ref[...]
    index = (reorder(index >> 8) * SPAN + reorder(index & (SPAN - 1))).astype(jnp.int32)
    lower = lax.broadcasted_iota(jnp.int32, (WIN_TOK, HALF), 0) % HALF < quarter
    ordered[0] = jnp.where(lower, index[:, :HALF], index[:, HALF:])
    ordered[1] = jnp.where(lower, index[:, HALF:], index[:, :HALF])
    steps = WIN_TOK // T_STEP
    spread = T_STEP * HALF
    for i in range(T_STEP):
        for other in range(2):
            start = other * spread + i * HALF
            idx_ref[:, start : start + HALF] = ordered[other, i * steps : (i + 1) * steps, :]

    lane = lax.broadcasted_iota(jnp.int32, (HALF, 128), 1)
    row = lax.broadcasted_iota(jnp.int32, (HALF, 128), 0)
    lane_head = lane // HEAD_DIM
    lat_start = lat * 2 * WIN_LAT
    same_level = (lane // quarter) == (row // quarter)
    same_rows = (lane // PIECE) % 2 == (row // PIECE) % 2
    lane_row = lane % quarter // WIN_LAT
    for b in range(2):
        wraps = lat_start + b * WIN_LAT >= lat_total - WIN_LAT
        usable = jnp.zeros((HALF, 128), jnp.int32)
        for r in range(WIN_LAT):
            value = pad_ref[lax.rem(lat_start + b * WIN_LAT + r + WIN_LAT // 2, lat_total)]
            usable = jnp.where(lane_row == r, value, usable)
        allowed = (lane < HALF) & (usable == 1) & jnp.logical_or(jnp.logical_not(wraps), same_rows)
        masks[0, b] = jnp.where(allowed, 1, 0)
        masks[1, b] = jnp.where(allowed & same_level, 1, 0)

    first_part = lax.broadcasted_iota(jnp.int32, (tables, 128), 1) < quarter
    width = 2 * spread

    def bias_rows(step, acc):
        def find(j):
            lanes = slice(j * 256, (j + 1) * 256)
            both = j * 256 < spread
            picked = idx_ref[step : step + 1, lanes]
            low = jnp.broadcast_to(picked & (SPAN - 1), (SPAN, 256))
            hot = jnp.where(lax.broadcasted_iota(jnp.int32, (SPAN, 256), 0) == low, 1.0, 0.0).astype(BF16)
            high = jnp.broadcast_to(picked >> 8, (tables, 256))
            entries = table_ref[...] if both else table_ref[:part_rows]
            found = jnp.dot(entries, hot, preferred_element_type=F32)
            for z in range(2 if both else 1):
                start = z * part_rows
                total = found[start : start + tables]
                for k in range(1, blocks):
                    total = jnp.where(high == k, found[start + k * tables : start + (k + 1) * tables], total)
                acc[z, :, lanes] = total

        def moved(z, source, target):
            base = source // 128 * 128
            shift = target - (source - base)
            if source - base + quarter <= 128:
                piece = acc[z, :, base : base + 128]
                return pltpu.roll(piece, shift % 128, 1) if shift % 128 else piece
            return pltpu.roll(acc[z, :, base : base + 256], shift % 256, 1)[:, :128]

        def keep_row(i):
            level = i // (T_STEP // 4) % 2
            for c in range(2):
                near = i * HALF + c * quarter
                same = moved(0, near, level * quarter)
                cross = moved(0, spread + near, (1 - level) * quarter)
                pair = (same, cross) if level == 0 else (cross, same)
                place = i * steps + step
                bias[c, pl.ds(place, tables, stride=WIN_TOK), :] = jnp.where(first_part, *pair)
                bias[c, pl.ds(tables * WIN_TOK + place, tables, stride=WIN_TOK), :] = moved(1, near, level * quarter)

        done = set()
        kept = 0
        for j in (0, 4, 5, 1, 6, 2, 7, 3, 8):
            find(j)
            done.add(j)
            while kept < T_STEP and all(
                p // 256 in done
                for start in (kept * HALF, spread + kept * HALF)
                for p in range(start, start + HALF)
            ):
                keep_row(kept)
                kept += 1

    edge_copy.wait_recv()
    for c in copiese:
        c.start()
    for c in copies0:
        c.start()

    for step in range(steps):
        bias_rows(step, acc.at[step])

    loads[4].wait()

    def rounded(x):
        return x.astype(BF16).astype(F32)

    def put_main(slot, both):
        for level in range(4):
            rolled = (level + 3) % 4
            start = (rolled % 2) * 2 * PIECE
            kv_buf[slot, rolled // 2, 0, start : start + 2 * PIECE, :] = both[
                level * 2 * PIECE : (level + 1) * 2 * PIECE
            ]

    def put_piece(slot, both, rh):
        for level in range(4):
            rolled = (level + 3) % 4
            start = (rolled % 2) * 2 * PIECE + rh * PIECE
            kv_buf[slot, rolled // 2, 1, start : start + PIECE, :] = both[level * PIECE : (level + 1) * PIECE]

    def put_query_main(half, both):
        for level in range(4):
            rolled = (level + 3) % 4
            start = (rolled % 2) * 2 * PIECE
            q_buf[half, rolled // 2, 0, start : start + 2 * PIECE, :] = both[
                level * 2 * PIECE : (level + 1) * 2 * PIECE
            ]

    def put_query(half, both, rh):
        for level in range(4):
            rolled = (level + 3) % 4
            start = (rolled % 2) * 2 * PIECE + rh * PIECE
            q_buf[half, rolled // 2, 1, start : start + PIECE, :] = both[level * PIECE : (level + 1) * PIECE]

    features = w_qkv.shape[0]
    own = jnp.concatenate(
        [ref[...].reshape(-1, features) for ref in (m0_ref, m1_ref, edge_in)], axis=0
    )
    full = rounded(jnp.dot(own, w_qkv[...], preferred_element_type=F32))
    for half in range(2):
        main = full[half * 2 * HALF : (half + 1) * 2 * HALF]
        put_query_main(half, main[:, :WIDTH])
        put_main(half + 1, main[:, WIDTH:])
        for rh in range(2):
            part = full[(4 + 2 * rh + half) * HALF : (5 + 2 * rh + half) * HALF]
            put_query(half, part[:, :WIDTH], rh)
            put_piece(half + 1, part[:, WIDTH:], rh)

    def attend(a, b, half):
        allowed = masks[a, b] == 1
        slot0 = 2 * half
        out = []
        zeros = jnp.zeros((128 - HALF, 128), F32)
        ones = jnp.ones((256, 128), BF16)
        query_half = 1 - half
        for g in range(GROUPS):
            cols = slice(g * 128, (g + 1) * 128)
            vcols = slice(WIDTH + g * 128, WIDTH + (g + 1) * 128)
            q = q_buf[half, a, b, :, cols]
            stacked = jnp.concatenate([jnp.where(lane_head == h, q, 0.0) for h in range(GROUP)], axis=0).astype(BF16)
            keys = jnp.concatenate(
                [kv_buf[slot0, a, b, :, cols], zeros, kv_buf[slot0 + 1, a, b, :, cols], zeros], axis=0
            ).astype(BF16)
            values = jnp.concatenate(
                [kv_buf[slot0, a, b, :, vcols], zeros, kv_buf[slot0 + 1, a, b, :, vcols], zeros], axis=0
            ).astype(BF16)
            values = jnp.concatenate([values, ones], axis=1)
            scores = nt_dot(stacked, keys)
            powers = []
            for h in range(GROUP):
                first = ((a * 2 + b) * HEADS + g * GROUP + h) * WIN_TOK + query_half * HALF
                parts = []
                for c in range(2):
                    s = scores[h * HALF : (h + 1) * HALF, c * 128 : (c + 1) * 128] * (HEAD_DIM**-0.5)
                    s = s + bias[c, pl.ds(pl.multiple_of(first, 8), HALF), :]
                    parts.append(jnp.where(allowed, s, NEG))
                largest = jnp.max(jnp.maximum(parts[0], parts[1]), axis=1, keepdims=True)
                powers.append(jnp.concatenate([jnp.exp(p - largest) for p in parts], axis=1))
            weights = jnp.concatenate(powers, axis=0).astype(BF16)
            product = jnp.dot(weights, values, preferred_element_type=F32)
            top = jnp.zeros((HALF, 128), F32)
            bottom = jnp.zeros((HALF, 128), F32)
            for h in range(GROUP):
                part = product[h * HALF : (h + 1) * HALF]
                top = jnp.where(lane_head == h, part[:, :128], top)
                bottom = jnp.where(lane_head == h, part[:, 128:], bottom)
            out.append(top / bottom)
        return jnp.concatenate(out, axis=1)

    for c in copies1 + copiese:
        c.wait_recv()
    other = jnp.concatenate([ref[...].reshape(-1, features) for ref in (halo1, haloe)], axis=0)
    full = rounded(jnp.dot(other, w_qkv[:, WIDTH:], preferred_element_type=F32))
    for c in range(2):
        for rh in range(2):
            put_piece(3 * c, full[(2 * rh + c) * HALF : (2 * rh + c + 1) * HALF], rh)

    def edge_unit(half):
        for a in range(2):
            result = attend(a, 1, half)
            for k in range(2):
                place = (2 * a + k + 1) % 4 * PIECE
                att1[half, place : place + PIECE, :] = result[2 * k * PIECE : (2 * k + 1) * PIECE]
                atte[half, place : place + PIECE, :] = result[(2 * k + 1) * PIECE : (2 * k + 2) * PIECE]

    for half in range(2):
        edge_unit(half)
    atte_out[...] = atte[...].astype(BF16)
    return_copy = remote(atte_out, atte_in, lat_send.at[1], lat_recv.at[1], partner)
    return_copy.start()

    for c in copies0:
        c.wait_recv()
    full = rounded(jnp.dot(halo0[...].reshape(-1, features), w_qkv[:, WIDTH:], preferred_element_type=F32))
    for c in range(2):
        put_main(3 * c, full[c * 2 * HALF : (c + 1) * 2 * HALF])

    def main_unit(half):
        for a in range(2):
            result = attend(a, 0, half)
            for k in range(2):
                place = (2 * a + k + 1) % 4 * 2 * PIECE
                att0[half, place : place + 2 * PIECE, :] = result[k * 2 * PIECE : (k + 1) * 2 * PIECE]

    for half in range(2):
        main_unit(half)
    for load in loads[5:]:
        load.wait()

    proj_bias, gain, shift = (ref[...][None] for ref in (proj_bias_ref, gain_ref, shift_ref))

    def finish(half, start, attended, hidden_ref):
        projected = jnp.dot(attended.astype(BF16), w_proj[...], preferred_element_type=F32)
        count = projected.shape[0]
        for first in range(0, count, NORM_ROWS):
            last = min(first + NORM_ROWS, count)
            part = projected[first:last] + proj_bias
            average = jnp.mean(part, axis=-1, keepdims=True)
            centered = part - average
            spread = jnp.mean(centered * centered, axis=-1, keepdims=True)
            normed = centered * lax.rsqrt(spread + norm_epsilon) * gain + shift
            total = hidden_ref[half, first:last].astype(F32) + normed
            for k in range(tokens.shape[1]):
                tokens[half, k, start + first : start + last, :] = total[:, k * 128 : (k + 1) * 128]

    def emit(row_range):
        for r in row_range:
            for half in range(2):
                for c in range(6):
                    place, step = place_of(r, half, c)
                    found = [tokens[half, k, pl.ds(place, levels, stride=step), :] for k in range(tokens.shape[1])]
                    out_ref[r, half * 6 + c] = jnp.concatenate(found, axis=1).astype(BF16)

    for half in range(2):
        finish(half, 0, att0[half], m0_ref)
        finish(half, 8 * PIECE, att1[half], m1_ref)
    emit(range(3, 12))
    stores = [
        pltpu.make_async_copy(out_ref.at[pl.ds(first, size)], out_hbm.at[pl.ds(first, size)], out_sem.at[k])
        for k, (first, size) in enumerate([(3, 9), (0, 3)])
    ]
    stores[0].start()
    return_copy.wait_recv()
    for half in range(2):
        finish(half, 12 * PIECE, atte_in[half], ed_ref)
    emit(range(3))
    stores[1].start()
    edge_copy.wait_send()
    return_copy.wait_send()
    for c in copies1 + copiese + copies0:
        c.wait_send()
    for store in stores:
        store.wait()


def on_device(
    state_tokens,
    land_mask,
    pad_mask,
    land_embed,
    w_qkv,
    w_proj,
    proj_bias,
    norm_gain,
    norm_shift,
    bias_table,
    index_table,
):
    levels, lat_rows, lon_columns, features = state_tokens.shape
    lat_windows, z_windows, heads, positions = bias_table.shape
    lat_total = lat_rows * lax.axis_size("lat")
    half_columns = WIN_LON // 2
    blocks = -(-positions // SPAN)

    side = (2, levels * PIECE, features)
    main = (2, levels * 2 * PIECE, features)
    rows = z_windows * lat_windows * heads
    table_rows = -(-blocks * lat_windows * heads // 16) * 16

    state = state_tokens.transpose(1, 2, 0, 3)
    tables = bias_table.transpose(0, 2, 1, 3)
    anywhere = pl.BlockSpec(memory_space=pl.ANY)
    smem = pl.BlockSpec(memory_space=pltpu.SMEM)
    result = pl.pallas_call(
        functools.partial(kernel, lat_total, blocks),
        out_shape=jax.ShapeDtypeStruct(state.shape, BF16),
        in_specs=[anywhere] * 9 + [smem] * 2,
        out_specs=anywhere,
        scratch_shapes=[
            pltpu.VMEM(state.shape, BF16),
            pltpu.VMEM(land_embed.shape, F32),
            pltpu.VMEM(index_table.shape, jnp.int32),
            pltpu.VMEM(tables.shape, BF16),
            pltpu.VMEM(proj_bias.shape, F32),
            pltpu.VMEM(norm_gain.shape, F32),
            pltpu.VMEM(norm_shift.shape, F32),
            pltpu.VMEM(state.shape, BF16),
            pltpu.VMEM((2, features // 128, 16 * PIECE, 128), F32),
            pltpu.VMEM(main, BF16),
            pltpu.VMEM(side, BF16),
            pltpu.VMEM(side, BF16),
            pltpu.VMEM((2, z_windows * table_rows, 128), F32),
            pltpu.VMEM((z_windows * table_rows, SPAN), BF16),
            pltpu.VMEM((2, WIN_TOK, HALF), jnp.int32),
            pltpu.VMEM((2, 2, HALF, 128), jnp.int32),
            pltpu.VMEM((WIN_TOK // T_STEP, T_STEP * WIN_TOK), jnp.int32),
            pltpu.VMEM(w_qkv.shape, BF16),
            pltpu.VMEM(w_proj.shape, BF16),
            pltpu.VMEM(side, BF16),
            pltpu.VMEM(main, BF16),
            pltpu.VMEM(side, BF16),
            pltpu.VMEM(side, BF16),
            pltpu.VMEM((2, 2, 2, HALF, WIDTH), F32),
            pltpu.VMEM((4, 2, 2, HALF, 2 * WIDTH), F32),
            pltpu.VMEM((WIN_TOK // T_STEP, 2, lat_windows * heads, T_STEP * WIN_TOK + 128), F32),
            pltpu.VMEM((2, rows * WIN_TOK, 128), F32),
            pltpu.VMEM((2, 2 * HALF, WIDTH), F32),
            pltpu.VMEM((2, HALF, WIDTH), F32),
            pltpu.VMEM((2, HALF, WIDTH), F32),
            pltpu.VMEM((2, HALF, WIDTH), BF16),
            pltpu.VMEM((2, HALF, WIDTH), BF16),
            pltpu.SemaphoreType.DMA((9,)),
            pltpu.SemaphoreType.DMA((2,)),
            pltpu.SemaphoreType.DMA((2,)),
            pltpu.SemaphoreType.DMA((2,)),
            pltpu.SemaphoreType.DMA((6,)),
            pltpu.SemaphoreType.DMA((6,)),
        ],
        compiler_params=pltpu.CompilerParams(
            collective_id=0, has_side_effects=True, vmem_limit_bytes=56 * 1024 * 1024
        ),
        name="window_layer",
    )(
        state,
        land_embed,
        index_table,
        tables,
        w_qkv,
        w_proj,
        proj_bias,
        norm_gain,
        norm_shift,
        land_mask,
        pad_mask,
    )
    return result.transpose(2, 0, 1, 3)


def solution(mesh):
    in_specs = (
        P("member", "lat", "lon", None),
        P("lat", "lon"),
        P(),
        P(),
        P(),
        P(),
        P(),
        P(),
        P(),
        P("lat", None, None, None),
        P(),
    )
    out_specs = P("member", "lat", "lon", None)
    return jax.shard_map(
        on_device, mesh=mesh, in_specs=in_specs, out_specs=out_specs, check_vma=False
    )
```
